32 devices in a mesh: coil: 4 (over z), spoke: 8 (over y, x, core).
Axes of the slice: x: 2, y: 2, z: 4, core: 2. Of those that a mesh axis runs over, the one named last changes fastest.
Arguments:
- image: float32 [256, 2, 2, 256], P('spoke'), may hold values from -6 to 6
- residual: float32 [256, 2, 2, 256], P('spoke'), may hold values from -12 to 12
- direction: float32 [256, 2, 2, 256], P('spoke'), may hold values from -12 to 12
- coil_maps: bfloat16 [256, 32, 2, 2, 256], P(None, 'coil'), may hold values from -0.75 to 0.75
- interp_weights: bfloat16 [64, 128, 2048], P('spoke'), may hold values from -0.125 to 0.125
- tile_index: int32 [64], P('spoke'), may hold values from 0 to 31
Outputs:
- new_image: float32 [256, 2, 2, 256], P('spoke')
- new_residual: float32 [256, 2, 2, 256], P('spoke')
- new_direction: float32 [256, 2, 2, 256], P('spoke')
The draws below stay inside these ranges and needn't reach their ends.
All inputs are finite; a program needn't handle non-finite values.
Results may differ from the reference program's by a relative error of at most 0.0017.
Values may be sent and summed in bfloat16 or wider, within the bound.
No kernel may reach another device: no remote copies, remote signals or barrier semaphores. Data moves between devices by JAX's collectives and lax.ppermute only.
A program may use at most 128 MiB of HBM per device.

```python
import math
import jax
import jax.numpy as jnp
from jax import lax

NY = 256
NX = 256
COILS = 32
PLANES = 2
TR = 8
SB = 128
NBLK = 8
BLOCKS = 64
TC = 2048
N_COIL = 4
N_SPOKE = 8


def rising_field(key):
    height = jnp.arange(NY, dtype=jnp.float32)[:, None, None, None] / (NY - 1)
    values = jnp.clip(jax.random.normal(key, (NY, PLANES, 2, NX), jnp.float32), -4.0, 4.0)
    return values * (1.0 + 2.0 * height)


def draw_residual(key, part):
    return rising_field(jax.random.fold_in(key, 17))


def draw_direction(key, part):
    return rising_field(jax.random.fold_in(key, 29))


def place_ends(drawn, stream_key, low, largest):
    shape = drawn.shape
    spot = [jax.random.randint(jax.random.fold_in(stream_key, axis), (), 0, shape[axis]) for axis in range(len(shape))]
    drawn = drawn.at[tuple(spot)].set(low)
    longest = shape.index(max(shape))
    spot[longest] = (spot[longest] + 1) % shape[longest]
    return drawn.at[tuple(spot)].set(largest)


def level_of(rng, extent, shards, low, high):
    factor_of, own = 1.0, jax.random.fold_in(rng, 6)
    for dim, parts in shards:
        steps = jnp.exp(jax.random.uniform(jax.random.fold_in(own, dim), (parts,), jnp.float32, low / len(shards), high / len(shards)))
        factor_of = factor_of * jnp.repeat(steps, extent[dim] // parts).reshape([-1 if axis == dim else 1 for axis in range(len(extent))])
    return factor_of


def normal_values(rng, dims, scale, limit, shards=(), kind=jnp.bfloat16):
    drawn = jax.random.normal(rng, dims, jnp.float32) * scale
    if len(shards) > 0:
        drawn = level_of(rng, dims, shards, -0.22, 0.18) * drawn
    return jnp.clip(drawn, min=-limit, max=limit).astype(kind)


def setup_inputs(seed: int = 0) -> dict:
    splits = jax.random.split(jax.random.key(seed), 7)
    image = normal_values(splits[0], (NY, PLANES, 2, NX), 1.0, 6.0, ((0, 8),), jnp.float32)
    residual = draw_residual(jax.random.fold_in(splits[6], 71), 0)
    direction = draw_direction(jax.random.fold_in(splits[6], 71), 0)
    coil_maps = normal_values(splits[3], (NY, COILS, PLANES, 2, NX), (2 * COILS) ** -0.5, 0.75, ((1, 4),))
    interp_weights = normal_values(splits[4], (BLOCKS, SB, TC), TC ** -0.5, 0.125, ((0, 8),))
    tile_index = place_ends(jax.random.randint(splits[5], (BLOCKS,), 0, NY // TR), jax.random.fold_in(splits[5], 1), 0, (NY // TR) - 1).astype(jnp.int32)
    return dict(image=image, residual=residual, direction=direction, coil_maps=coil_maps, interp_weights=interp_weights, tile_index=tile_index)


ridge = 0.1

def wave_tables(first, second, length):
    phase = first[:, None] * second[None, :] % length
    angle = phase.astype(jnp.float32) * (2.0 * math.pi / length)
    factor = 1.0 / math.sqrt(length)
    return ((jnp.cos(angle) * factor).astype(jnp.bfloat16), (jnp.sin(angle) * factor).astype(jnp.bfloat16))

def row_tables():
    lines = jnp.arange(NX, dtype=jnp.int32)
    cosines, sines = wave_tables(lines, lines, NX)
    forward_row = jnp.concatenate([jnp.concatenate([cosines, -sines], 1), jnp.concatenate([sines, cosines], 1)], 0)
    inverse_row = jnp.concatenate([jnp.concatenate([cosines, sines], 1), jnp.concatenate([-sines, cosines], 1)], 0)
    return (forward_row, inverse_row)

def coil_spectra(maps_rows, field_rows, forward_row):
    maps_real = maps_rows[..., 0, :].astype(jnp.float32)
    maps_imag = maps_rows[..., 1, :].astype(jnp.float32)
    field_real = field_rows[:, None, :, 0, :]
    field_imag = field_rows[:, None, :, 1, :]
    coil_real = maps_real * field_real - maps_imag * field_imag
    coil_imag = maps_real * field_imag + maps_imag * field_real
    coil_image = jnp.stack([coil_real, coil_imag], -2).astype(jnp.bfloat16)
    spectra = jnp.dot(coil_image.reshape(-1, 2 * NX), forward_row, preferred_element_type=jnp.float32)
    return spectra.astype(jnp.bfloat16).reshape(coil_image.shape)

def combine_coils(maps_rows, images):
    maps_real = maps_rows[..., 0, :].astype(jnp.float32)
    maps_imag = maps_rows[..., 1, :].astype(jnp.float32)
    image_real = images[..., 0, :]
    image_imag = images[..., 1, :]
    combined_real = lax.optimization_barrier(jnp.sum(maps_real * image_real + maps_imag * image_imag, axis=1))
    combined_imag = lax.optimization_barrier(jnp.sum(maps_real * image_imag - maps_imag * image_real, axis=1))
    return jnp.stack([combined_real, combined_imag], -2)

def reference(image, residual, direction, coil_maps, interp_weights, tile_index):
    forward_row, inverse_row = row_tables()
    lines = jnp.arange(NY, dtype=jnp.int32)
    cosines, sines = wave_tables(lines, lines, NY)
    group_coils = COILS // N_COIL
    flat_width = group_coils * PLANES * 2 * NX
    block_index = tile_index.reshape(N_SPOKE, NBLK).astype(jnp.int32)
    block_weights = interp_weights.reshape(N_SPOKE, NBLK, SB, TR, NX)
    combined = jnp.zeros((NY, PLANES, 2, NX), jnp.float32)
    for group in range(N_COIL):
        maps_group = coil_maps[:, group * group_coils:(group + 1) * group_coils]
        spectra = coil_spectra(maps_group, direction, forward_row).reshape(NY, flat_width)
        first = jnp.dot(cosines, spectra, preferred_element_type=jnp.float32).reshape(NY, group_coils, PLANES, 2, NX)
        second = jnp.dot(sines, spectra, preferred_element_type=jnp.float32).reshape(NY, group_coils, PLANES, 2, NX)
        kspace = jnp.stack([first[..., 0, :] + second[..., 1, :], first[..., 1, :] - second[..., 0, :]], -2)
        kspace = kspace.astype(jnp.bfloat16).reshape(NY // TR, TR, group_coils, PLANES, 2, NX)

        def grid_device(total, inputs):
            indices, weights = inputs
            picked = kspace[indices].astype(jnp.float32)
            weights_wide = weights.astype(jnp.float32)
            samples = jnp.einsum('btcpax,bjtx->bcpaj', picked, weights_wide, precision=lax.Precision.HIGHEST)
            samples = samples.astype(jnp.bfloat16).astype(jnp.float32)
            gridded = jnp.einsum('bcpaj,bjtx->btcpax', samples, weights_wide, precision=lax.Precision.HIGHEST)
            gridded = gridded.astype(jnp.bfloat16)
            spread = jnp.dot(gridded.reshape(-1, 2 * NX), inverse_row, preferred_element_type=jnp.float32)
            spread = spread.astype(jnp.bfloat16).astype(jnp.float32).reshape(NBLK, TR, group_coils, PLANES, 2, NX)
            return (total.at[indices].add(spread), None)
        start_total = jnp.zeros((NY // TR, TR, group_coils, PLANES, 2, NX), jnp.float32)
        gridded_total, unused = lax.scan(grid_device, start_total, (block_index, block_weights))
        gridded_total = gridded_total.reshape(NY, flat_width)
        first = jnp.dot(cosines.astype(jnp.float32), gridded_total, precision=lax.Precision.HIGHEST)
        second = jnp.dot(sines.astype(jnp.float32), gridded_total, precision=lax.Precision.HIGHEST)
        first = first.reshape(NY, group_coils, PLANES, 2, NX)
        second = second.reshape(NY, group_coils, PLANES, 2, NX)
        images = jnp.stack([first[..., 0, :] - second[..., 1, :], first[..., 1, :] + second[..., 0, :]], -2)
        combined = combined + combine_coils(maps_group, images)
    applied = combined + ridge * direction
    norm_now = jnp.sum(residual * residual)
    alpha = norm_now / jnp.sum(direction * applied)
    new_image = image + alpha * direction
    new_residual = residual - alpha * applied
    norm_next = jnp.sum(new_residual * new_residual)
    new_direction = new_residual + norm_next / norm_now * direction
    return (new_image, new_residual, new_direction)
```

```python
import math

import jax
import jax.numpy as jnp
import numpy as np
from jax import lax
from jax.experimental import pallas as pl
from jax.experimental.pallas import tpu as pltpu
from jax.sharding import PartitionSpec as P

ridge = 0.1


def wave_table(length):
    lines = np.arange(length, dtype=np.int64)
    phase = lines[:, None] * lines[None, :] % length
    angle = phase.astype(np.float64) * (2.0 * math.pi / length)
    factor = 1.0 / math.sqrt(length)
    rounded = [(wave(angle) * factor).astype(np.float32).astype(jnp.bfloat16) for wave in (np.cos, np.sin)]
    return rounded


def row_tables(length):
    cosines, sines = wave_table(length)
    forward_row = np.concatenate(
        [np.concatenate([cosines, -sines], 1), np.concatenate([sines, cosines], 1)], 0
    )
    inverse_row = np.concatenate(
        [np.concatenate([cosines, sines], 1), np.concatenate([-sines, cosines], 1)], 0
    )
    return forward_row, inverse_row


def swap(value, axis, size, step):
    return lax.ppermute(value, axis, [(i, i ^ step) for i in range(size)])


def tree_sum(values):
    while len(values) > 1:
        values = [values[i] + values[i + 1] for i in range(0, len(values), 2)]
    return values[0]


def make_kernel(spokes, row_count, coils, planes, width, blocks, tile_rows, spots):
    height = spokes * row_count
    pairs = coils * planes
    waves = blocks * tile_rows
    lanes = 128
    quarters = 2 * width // lanes
    chunk = 32
    f32 = jnp.float32
    bf16 = jnp.bfloat16

    def kernel(place, tiles, *refs):
        fields = refs[:spokes]
        maps, weights_hbm, cosines, sines, forward_row, inverse_row = refs[spokes : spokes + 6]
        outs = refs[spokes + 6 : 2 * spokes + 6]
        weights, arrived, field, tall, images, lines, turned, gridded, sums, combined = refs[
            2 * spokes + 6 :
        ]
        copies = [
            pltpu.make_async_copy(weights_hbm.at[b], weights.at[b], arrived.at[b])
            for b in range(blocks)
        ]
        for copy in copies:
            copy.start()
        own = place[0]
        for k in range(spokes):
            start = pl.multiple_of((own ^ k) * row_count, row_count)
            field[pl.ds(start, row_count), :] = fields[k][...].astype(f32)
        for b in range(blocks):
            start = pl.multiple_of(tiles[b] * tile_rows, tile_rows)
            cos_rows = cosines[pl.ds(start, tile_rows), :]
            sin_rows = sines[pl.ds(start, tile_rows), :]
            low = b * tile_rows
            tall[low : low + tile_rows, :height] = cos_rows
            tall[low : low + tile_rows, height:] = sin_rows
            tall[waves + low : waves + low + tile_rows, :height] = -sin_rows
            tall[waves + low : waves + low + tile_rows, height:] = cos_rows

        def make_images(step, carry):
            start = pl.multiple_of(step * chunk, chunk)
            rows = pl.ds(start, chunk)
            rows_imag = pl.ds(pl.multiple_of(height + start, chunk), chunk)
            for p in range(planes):
                field_real = field[rows, 2 * p * width : (2 * p + 1) * width]
                field_imag = field[rows, (2 * p + 1) * width : (2 * p + 2) * width]
                for c in range(coils):
                    i = c * planes + p
                    real = maps[2 * i, rows, :].astype(f32)
                    imag = maps[2 * i + 1, rows, :].astype(f32)
                    images[rows, i * width : (i + 1) * width] = (
                        real * field_real - imag * field_imag
                    ).astype(bf16)
                    images[rows_imag, i * width : (i + 1) * width] = (
                        real * field_imag + imag * field_real
                    ).astype(bf16)
            return carry

        lax.fori_loop(0, height // chunk, make_images, 0)
        tall_bf = tall[...].astype(bf16)
        for i in range(pairs):
            column = jnp.dot(
                tall_bf, images[:, i * width : (i + 1) * width], preferred_element_type=f32
            ).astype(bf16)
            lines[i * waves : (i + 1) * waves, :width] = column[:waves]
            lines[i * waves : (i + 1) * waves, width:] = column[waves:]
        group = 4
        for i in range(0, pairs, group):
            spectrum = jnp.dot(
                lines[i * waves : (i + group) * waves, :],
                forward_row[...],
                preferred_element_type=f32,
            )
            for g in range(group):
                for q in range(quarters):
                    turned[q, pl.ds(i + g, waves, stride=pairs), :] = spectrum[
                        g * waves : (g + 1) * waves, q * lanes : (q + 1) * lanes
                    ]
        half = quarters // 2
        for b in range(blocks):
            copies[b].wait()
            real = []
            imag = []
            for r in range(tile_rows):
                low = (b * tile_rows + r) * pairs
                for q in range(half):
                    real.append(turned[q, low : low + pairs, :].astype(bf16))
                    imag.append(turned[half + q, low : low + pairs, :].astype(bf16))
            picked = jnp.concatenate(
                [jnp.concatenate(real, axis=1), jnp.concatenate(imag, axis=1)], axis=0
            )
            samples = lax.dot_general(
                picked, weights[b], (((1,), (1,)), ((), ())), preferred_element_type=f32
            ).astype(bf16)
            back = jnp.dot(samples, weights[b], preferred_element_type=f32).astype(bf16)
            for r in range(tile_rows):
                low = (b * tile_rows + r) * pairs
                gridded[low : low + pairs, :width] = back[:pairs, r * width : (r + 1) * width]
                gridded[low : low + pairs, width:] = back[pairs:, r * width : (r + 1) * width]
        for b in range(blocks):
            low = b * tile_rows * pairs
            high = low + tile_rows * pairs
            spread = jnp.dot(
                gridded[low:high, :], inverse_row[...], preferred_element_type=f32
            )
            for q in range(quarters):
                turned[q, low:high, :] = spread[:, q * lanes : (q + 1) * lanes]
        back_table = tall[...].T.astype(bf16)
        for i in range(pairs):
            parts = [
                turned[q, pl.ds(i, waves, stride=pairs), :].astype(bf16) for q in range(quarters)
            ]
            stacked = jnp.concatenate(
                [jnp.concatenate(parts[:half], axis=1), jnp.concatenate(parts[half:], axis=1)],
                axis=0,
            )
            sums[:, i * width : (i + 1) * width] = jnp.dot(
                back_table, stacked, preferred_element_type=f32
            )

        def combine(step, carry):
            start = pl.multiple_of(step * chunk, chunk)
            rows = pl.ds(start, chunk)
            rows_imag = pl.ds(pl.multiple_of(height + start, chunk), chunk)
            for p in range(planes):
                total_real = jnp.zeros((chunk, width), f32)
                total_imag = jnp.zeros((chunk, width), f32)
                for c in range(coils):
                    i = c * planes + p
                    real = maps[2 * i, rows, :].astype(f32)
                    imag = maps[2 * i + 1, rows, :].astype(f32)
                    image_real = sums[rows, i * width : (i + 1) * width]
                    image_imag = sums[rows_imag, i * width : (i + 1) * width]
                    total_real += real * image_real + imag * image_imag
                    total_imag += real * image_imag - imag * image_real
                combined[rows, 2 * p * width : (2 * p + 1) * width] = total_real
                combined[rows, (2 * p + 1) * width : (2 * p + 2) * width] = total_imag
            return carry

        lax.fori_loop(0, height // chunk, combine, 0)
        for k in range(spokes):
            start = pl.multiple_of((own ^ k) * row_count, row_count)
            outs[k][...] = combined[pl.ds(start, row_count), :].astype(bf16)

    flat = planes * 2 * width
    smem = pl.BlockSpec(memory_space=pltpu.SMEM)
    vmem = pl.BlockSpec(memory_space=pltpu.VMEM)
    return pl.pallas_call(
        kernel,
        out_shape=[jax.ShapeDtypeStruct((row_count, flat), bf16)] * spokes,
        in_specs=[smem, smem]
        + [vmem] * spokes
        + [vmem, pl.BlockSpec(memory_space=pl.ANY)]
        + [vmem] * 4,
        out_specs=[vmem] * spokes,
        scratch_shapes=[
            pltpu.VMEM((blocks, spots, tile_rows * width), bf16),
            pltpu.SemaphoreType.DMA((blocks,)),
            pltpu.VMEM((height, flat), f32),
            pltpu.VMEM((2 * waves, 2 * height), f32),
            pltpu.VMEM((2 * height, pairs * width), bf16),
            pltpu.VMEM((pairs * waves, 2 * width), bf16),
            pltpu.VMEM((quarters, waves * pairs, lanes), f32),
            pltpu.VMEM((waves * pairs, 2 * width), bf16),
            pltpu.VMEM((2 * height, pairs * width), f32),
            pltpu.VMEM((height, flat), f32),
        ],
        compiler_params=pltpu.CompilerParams(vmem_limit_bytes=56 * 1024 * 1024),
    )


def apply_kernel(owned, other, direction, residual, applied, inner):
    field = direction[...]
    rest = residual[...]
    total = owned[...] + other[...] + ridge * field
    applied[...] = total
    inner[...] = jnp.zeros(inner.shape, jnp.float32)
    products = (rest * rest, field * total, rest * total, total * total)
    for n, product in enumerate(products):
        line = jnp.sum(product, axis=0, keepdims=True)
        lanes = inner.shape[1]
        inner[n : n + 1, :] = sum(
            line[:, i : i + lanes] for i in range(0, line.shape[1], lanes)
        )


def update_kernel(inner, applied, image, residual, direction, new_image, new_residual, new_direction):
    norm_now, curvature, crossing, squared = (
        jnp.sum(inner[n : n + 1, :], axis=1, keepdims=True) for n in range(4)
    )
    alpha = norm_now / curvature
    norm_next = norm_now - 2.0 * alpha * crossing + alpha * alpha * squared
    beta = norm_next / norm_now
    field = direction[...]
    rest = residual[...] - alpha * applied[...]
    new_image[...] = image[...] + alpha * field
    new_residual[...] = rest
    new_direction[...] = rest + beta * field


def shards(image, residual, direction, coil_maps, interp_weights, tile_index):
    spokes = lax.axis_size("spoke")
    groups = lax.axis_size("coil")
    row_count, planes, _, width = direction.shape
    height, coils = coil_maps.shape[:2]
    blocks, spots, cells = interp_weights.shape
    tile_rows = cells // width
    flat = planes * 2 * width
    cosines, sines = wave_table(height)
    forward_row, inverse_row = row_tables(width)
    shape = direction.shape
    image, residual, direction = (v.reshape(row_count, flat) for v in (image, residual, direction))
    sent = direction.astype(jnp.bfloat16)
    place = lax.axis_index("spoke").astype(jnp.int32).reshape(1)
    direct = spokes in (2, 4, 8) and row_count % 8 == 0
    slots = spokes if direct else 1
    if direct:
        fields = [sent] + [swap(sent, "spoke", spokes, k) for k in range(1, spokes)]
    else:
        fields = [lax.all_gather(sent, "spoke", axis=0, tiled=True)]
        place = place * 0
    parts = make_kernel(slots, height // slots, coils, planes, width, blocks, tile_rows, spots)(
        place,
        tile_index,
        *fields,
        coil_maps.transpose(1, 2, 3, 0, 4).reshape(-1, height, width),
        interp_weights,
        jnp.asarray(cosines.astype(np.float32)),
        jnp.asarray(sines.astype(np.float32)),
        jnp.asarray(forward_row),
        jnp.asarray(inverse_row),
    )
    if direct:
        received = [parts[0]] + [swap(parts[k], "spoke", spokes, k) for k in range(1, spokes)]
        owned = tree_sum([v.astype(jnp.float32) for v in received])
    else:
        owned = lax.psum_scatter(
            parts[0].astype(jnp.float32), "spoke", scatter_dimension=0, tiled=True
        )
    other = jnp.zeros_like(owned)
    if groups in (2, 4, 8):
        step = 1
        while step < groups:
            owned = owned + other
            other = swap(owned, "coil", groups, step)
            step *= 2
    else:
        owned = lax.psum(owned, "coil")
    applied, inner = pl.pallas_call(
        apply_kernel,
        out_shape=[
            jax.ShapeDtypeStruct((row_count, flat), jnp.float32),
            jax.ShapeDtypeStruct((8, 128), jnp.float32),
        ],
    )(owned, other, direction, residual)
    if direct:
        step = 1
        while step < spokes:
            inner = inner + swap(inner, "spoke", spokes, step)
            step *= 2
    else:
        inner = lax.psum(inner, "spoke")
    news = pl.pallas_call(
        update_kernel, out_shape=[jax.ShapeDtypeStruct((row_count, flat), jnp.float32)] * 3
    )(inner, applied, image, residual, direction)
    return tuple(v.reshape(shape) for v in news)


def solution(mesh):
    rows = P("spoke", None, None, None)
    in_specs = (
        rows,
        rows,
        rows,
        P(None, "coil", None, None, None),
        P("spoke", None, None),
        P("spoke"),
    )
    return jax.shard_map(
        shards, mesh=mesh, in_specs=in_specs, out_specs=(rows, rows, rows), check_vma=False
    )
```
